256 devices in a mesh: slices: 2 (over z), wide: 16 (over y, core), narrow: 8 (over x).
Axes of the slice: x: 8, y: 8, z: 2, core: 2. Of those that a mesh axis runs over, the one named last changes fastest.
The devices are a block of a 8x8x16 slice.
Arguments:
- state: float32 [32, 8, 2, 16384], P(('slices', 'wide'), 'narrow'), parts along dimension 0, may hold values from -6 to 6
- gates: float32 [8, 7, 2, 4, 4], replicated, may hold values from -2 to 2
Outputs:
- final_state: float32 [32, 8, 2, 16384], P(('slices', 'wide'), 'narrow'), parts along dimension 0
- marginal: float32 [32, 16384], P(('slices', 'wide'), 'narrow'), parts along dimension 0
The draws below stay inside these ranges and needn't reach their ends.
There are 2 independent parts, one for each index of `slices`. The reference program is written for one: setup_inputs(seed, part) draws one part's arguments, and reference() takes and returns one part's arrays. A program takes and returns all parts, laid end to end along the dimension named above; an argument that names none is the same for every part. Nothing has to cross between parts.
All inputs are finite; a program needn't handle non-finite values.
Results may differ from the reference program's by a relative error of at most 0.0003.
Values sent between devices are 32-bit elements; how exact they have to be, the bound alone decides.
No kernel may reach another device: no remote copies, remote signals or barrier semaphores. Data moves between devices by JAX's collectives and lax.ppermute only.
A program may use at most 192 MiB of HBM per device.

```python
import jax
import jax.numpy as jnp
from jax import lax

LAYERS = 8
AMP_DEV = 16384
PAIRS = 7
N_WIDE = 16
N_NARROW = 8


def steps_of(stream_key, dims, shards, low, largest):
    factor_of, own = 1.0, jax.random.fold_in(stream_key, 6)
    for axis_at, blocks in shards:
        heights = jnp.exp(jax.random.uniform(jax.random.fold_in(own, axis_at), (blocks,), jnp.float32, low / len(shards), largest / len(shards)))
        factor_of = factor_of * jnp.repeat(heights, dims[axis_at] // blocks).reshape([-1 if axis == axis_at else 1 for axis in range(len(dims))])
    return factor_of


def noise(stream_key, dims, deviation, most, shards=(), kind=jnp.bfloat16):
    drawn = deviation * jax.random.normal(stream_key, dims, jnp.float32)
    if shards:
        drawn = drawn * steps_of(stream_key, dims, shards, -0.22, 0.18)
    return jnp.clip(drawn, -most, most).astype(kind)


def setup_inputs(seed: int = 0, part: int = 0) -> dict:
    key_list = jax.random.split(jax.random.key(seed), 3)
    part_keys = jax.random.split(jax.random.fold_in(key_list[2], part), 3)
    state = noise(part_keys[0], (N_WIDE, N_NARROW, 2, AMP_DEV), 1.0, 6.0, ((0, 16), (1, 8)), jnp.float32)
    gates = noise(key_list[1], (LAYERS, PAIRS, 2, 4, 4), 8 ** -0.5, 2.0, (), jnp.float32)
    return {"state": state, "gates": gates}


BIT_LETTERS = "abdefghjklmnpqrstuvwxyzABCDEFGHIJKLM"


def apply_gate(psi, gate, low_label, high_label, total_bits):
    letters = BIT_LETTERS[:total_bits]
    low_pos = total_bits - 1 - low_label
    high_pos = total_bits - 1 - high_label
    source = "i" + letters
    target_list = list(letters)
    target_list[high_pos] = "W"
    target_list[low_pos] = "X"
    target = "o" + "".join(target_list)
    real_part = gate[0]
    imag_part = gate[1]
    block = jnp.stack([jnp.stack([real_part, -imag_part]), jnp.stack([imag_part, real_part])])
    block = block.reshape(2, 2, 2, 2, 2, 2)
    gate_form = "oiWX" + letters[high_pos] + letters[low_pos]
    return jnp.einsum(gate_form + "," + source + "->" + target, block, psi, precision=lax.Precision.HIGHEST)


def reference(state, gates):
    high_bits = (N_WIDE * N_NARROW).bit_length() - 1
    local_bits = AMP_DEV.bit_length() - 1
    total_bits = local_bits + high_bits
    psi = jnp.transpose(state, (2, 0, 1, 3)).reshape((2,) + (2,) * total_bits)
    for layer_index in range(LAYERS):
        start = layer_index * high_bits
        for pair_index in range(local_bits // 2):
            low_label = (start + 2 * pair_index) % total_bits
            high_label = (start + 2 * pair_index + 1) % total_bits
            psi = apply_gate(psi, gates[layer_index, pair_index], low_label, high_label, total_bits)
    offset = ((LAYERS - 1) * high_bits) % total_bits
    axes_order = [0] + [1 + total_bits - 1 - ((offset + place) % total_bits) for place in range(total_bits - 1, -1, -1)]
    final = jnp.transpose(psi, axes_order).reshape(2, N_WIDE, N_NARROW, AMP_DEV)
    prob = final[0] * final[0] + final[1] * final[1]
    marginal = jnp.sum(prob, axis=1)
    return jnp.transpose(final, (1, 2, 0, 3)), marginal
```

```python
import jax
import jax.numpy as jnp
from jax import lax
from jax.experimental import pallas as pl
from jax.experimental.pallas import tpu as pltpu
from jax.sharding import Mesh, PartitionSpec as P

RING = 21
STEP = 7
VREGS = 16
SUBLANES = 8
LANES = 128
TILE = (SUBLANES, LANES)


def pair_of(layer, low):
    return layer, ((low - layer * STEP) % RING) // 2


def lane_iota():
    return lax.broadcasted_iota(jnp.int32, TILE, 1)


def sublane_iota():
    return lax.broadcasted_iota(jnp.int32, TILE, 0)


def bit_of(array, place):
    return (array >> place) & 1


def splits(array):
    high = array.astype(jnp.bfloat16)
    low = (array - high.astype(jnp.float32)).astype(jnp.bfloat16)
    return high, low


def dot(a, b, dims):
    return lax.dot_general(a, b, (dims, ((), ())), preferred_element_type=jnp.float32)


def dot_three(a, b, dims):
    return dot(a[0], b[0], dims) + dot(a[0], b[1], dims) + dot(a[1], b[0], dims)


def stack(parts):
    return jnp.concatenate(parts, axis=0)


def beside(left, right):
    return tuple(jnp.concatenate([l, r], axis=1) for l, r in zip(left, right))


def over(top, bottom):
    return tuple(jnp.concatenate([t, b], axis=0) for t, b in zip(top, bottom))


def negative(parts):
    return tuple(-part for part in parts)


def unstack(array):
    return [array[SUBLANES * v : SUBLANES * (v + 1)] for v in range(array.shape[0] // SUBLANES)]


def times_from_left(matrix, real, imag):
    left = beside(splits(matrix[0]), splits(matrix[1]))
    re, im = splits(real), splits(imag)
    right = over(beside(re, im), beside(negative(im), re))
    out = dot_three(left, right, ((1,), (0,)))
    return out[:, :LANES], out[:, LANES:]


def lane_operator(matrix):
    re, im = splits(matrix[0]), splits(matrix[1])
    return over(beside(re, negative(im)), beside(im, re))


def times_on_lanes(operator, real, imag):
    out = dot_three(beside(splits(real), splits(imag)), operator, ((1,), (1,)))
    return out[:, :LANES], out[:, LANES:]


def times_on_lanes_transposed(operator, real, imag):
    out = dot_three(operator, beside(splits(real), splits(imag)), ((1,), (1,)))
    return out[:LANES], out[LANES:]


def table_of(gates_ref, scratch, layer, pair):
    at = 2 * (layer * gates_ref.shape[0] // 16 + pair)
    scratch[0:4, 0:4] = gates_ref[at]
    scratch[4:8, 0:4] = gates_ref[at + 1]
    return scratch[...]


def spread(tile, row):
    return jnp.broadcast_to(tile[row : row + 1, :], TILE)


def brick(gates, ins, outs):
    lane, sub = lane_iota(), sublane_iota()
    touched, factors = set(), []
    for table, low in gates:
        high = (low + 1) % RING
        touched |= {low, high}
        column = bit_of(lane, ins[low]) + 2 * bit_of(lane, ins[high])
        wide = jnp.take_along_axis(table, column, axis=1)
        factors.append((low, high, [(spread(wide, r), spread(wide, 4 + r)) for r in range(4)]))
    cache = {}

    def static(place, v):
        return None if place < 3 else (v >> (place - 3)) & 1

    def pick(place, v, zero, one):
        if place >= 3:
            return one if static(place, v) else zero
        mask = bit_of(sub, place) == 1
        return tuple(jnp.where(mask, o, z) for z, o in zip(zero, one))

    def entry(index, v):
        low, high, rows = factors[index]
        key = (index, static(outs[low], v), static(outs[high], v))
        if key not in cache:
            zero = pick(outs[low], v, rows[0], rows[1])
            one = pick(outs[low], v, rows[2], rows[3])
            cache[key] = pick(outs[high], v, zero, one)
        return cache[key], key

    real, imag = [], []
    for v in range(VREGS):
        value, key = entry(0, v)
        key = (key,)
        for index in range(1, len(factors)):
            other, own = entry(index, v)
            key = key + (own,)
            if key not in cache:
                (a, b), (c, d) = value, other
                cache[key] = (a * c - b * d, a * d + b * c)
            value = cache[key]
        mask = None
        for qubit in ins:
            if qubit in touched:
                continue
            place = outs[qubit]
            bit = bit_of(lane, ins[qubit])
            same = (bit == bit_of(sub, place)) if place < 3 else (bit == static(place, v))
            mask = same if mask is None else mask & same
        if mask is not None:
            value = tuple(jnp.where(mask, part, 0.0) for part in value)
        real.append(value[0])
        imag.append(value[1])
    return stack(real), stack(imag)


def product(layers, places, get, outs=None):
    matrix = None
    for number, layer in enumerate(layers):
        last = number == len(layers) - 1
        step = brick([(get(*g), g[1]) for g in layer], places, outs if outs and last else places)
        matrix = step if matrix is None else times_from_left(step, *matrix)
    return matrix


def flip_lanes(tile, place):
    width = 1 << place
    if 2 * width == LANES:
        return pltpu.roll(tile, width, 1)
    lane = lane_iota()
    return jnp.where(bit_of(lane, place) == 1, pltpu.roll(tile, width, 1), pltpu.roll(tile, LANES - width, 1))


def flip_rows(tiles, place):
    if place >= 3:
        return [tiles[v ^ (1 << (place - 3))] for v in range(VREGS)]
    width = 1 << place
    up = bit_of(sublane_iota(), place) == 1
    return [jnp.where(up, pltpu.roll(t, width, 0), pltpu.roll(t, SUBLANES - width, 0)) for t in tiles]


def cross(real, imag, table, lane_place, row_place, lane_is_low):
    lane, sub = lane_iota(), sublane_iota()
    lane_bit = bit_of(lane, lane_place)
    lane_weight, row_weight = (1, 2) if lane_is_low else (2, 1)

    def coefficient(row_value, row_flip, lane_flip):
        column = lane_weight * (lane_bit ^ lane_flip) + row_weight * (row_value ^ row_flip)
        wide = jnp.take_along_axis(table, column, axis=1)
        base = row_weight * row_value
        return tuple(
            jnp.where(lane_bit == 1, spread(wide, shift + base + lane_weight), spread(wide, shift + base))
            for shift in (0, 4)
        )

    def coefficients(row_value):
        return {(r, l): coefficient(row_value, r, l) for r in (0, 1) for l in (0, 1)}

    both = [coefficients(0), coefficients(1)]
    if row_place < 3:
        mask = bit_of(sub, row_place) == 1
        mixed = {k: tuple(jnp.where(mask, o, z) for z, o in zip(both[0][k], both[1][k])) for k in both[0]}
    inputs = {}
    for l in (0, 1):
        re = [flip_lanes(t, lane_place) for t in real] if l else real
        im = [flip_lanes(t, lane_place) for t in imag] if l else imag
        for r in (0, 1):
            inputs[r, l] = (flip_rows(re, row_place), flip_rows(im, row_place)) if r else (re, im)
    out_real, out_imag = [], []
    for v in range(VREGS):
        factors = mixed if row_place < 3 else both[(v >> (row_place - 3)) & 1]
        re = im = None
        for key, (c, d) in factors.items():
            a, b = inputs[key][0][v], inputs[key][1][v]
            re = a * c - b * d if re is None else re + a * c - b * d
            im = a * d + b * c if im is None else im + a * d + b * c
        out_real.append(re)
        out_imag.append(im)
    return out_real, out_imag


def exchanged(tiles, pairs):
    lane = lane_iota()
    for register, place in pairs:
        width = 1 << place
        upper = bit_of(lane, place) == 1
        result = list(tiles)
        for v in range(VREGS):
            if (v >> register) & 1:
                continue
            other = v | (1 << register)
            a, b = tiles[v], tiles[other]
            result[v] = jnp.where(upper, pltpu.roll(b, width, 1), a)
            result[other] = jnp.where(upper, b, pltpu.roll(a, LANES - width, 1))
        tiles = result
    return tiles


def places_of(qubits):
    return {q: place for place, q in enumerate(qubits)}


LANES_ONE, ROWS_ONE = places_of(range(0, 7)), places_of(range(7, 14))
LANES_TWO, ROWS_TWO = places_of([0, 1, 2, 3, 20, 19, 18]), places_of([14, 15, 16, 13, 12, 11, 17])
LANES_THREE, LANES_LAST = places_of([7, 8, 9, 13, 12, 11, 10]), places_of(range(7, 14))


def layers_of(*layers):
    return [[(layer, low) for layer, low in group] for group in layers]


A_ONE = layers_of(
    [(0, 0), (0, 2), (0, 4)], [(2, 1), (2, 3), (2, 5)], [(3, 2), (3, 4)], [(5, 3)]
)
B_ONE = layers_of(
    [(0, 8), (0, 10), (0, 12)], [(1, 7), (1, 9), (1, 11)], [(3, 8), (3, 10)], [(4, 9)]
)
A_ONE_LATE = layers_of([(5, 5)], [(6, 4)])
B_ONE_LATE = layers_of([(4, 7)], [(6, 8)])
A_TWO = layers_of([(1, 19)], [(2, 18), (2, 20)], [(4, 19), (3, 0)])
B_TWO = layers_of(
    [(1, 13), (1, 15)], [(2, 14), (2, 16), (3, 12)], [(4, 11), (4, 13), (4, 15)]
)
A_TWO_LATE = layers_of([(5, 18), (5, 20), (5, 1)], [(7, 19), (6, 0), (6, 2)])
B_TWO_LATE = layers_of([(5, 14), (5, 16), (6, 12)], [(7, 13), (7, 15)])
D_THREE = layers_of([(6, 10)], [(7, 9), (7, 11), (7, 7)])


def getter(gates_ref, scratch):
    def get(layer, low):
        return table_of(gates_ref, scratch, *pair_of(layer, low))

    return get


def pair_op(op, matrix, real, imag):
    re, im = op(matrix, stack(real), stack(imag))
    return unstack(re), unstack(im)


def stage_one(x_ref, gates_ref, out_ref, scratch):
    get = getter(gates_ref, scratch)
    real = [x_ref[pl.ds(16 * v, SUBLANES, stride=2), :] for v in range(VREGS)]
    imag = [x_ref[pl.ds(16 * v + 1, SUBLANES, stride=2), :] for v in range(VREGS)]
    real, imag = cross(real, imag, get(0, 6), 6, 0, True)
    real, imag = pair_op(times_on_lanes, lane_operator(product(A_ONE, LANES_ONE, get)), real, imag)
    real, imag = pair_op(times_from_left, product(B_ONE, ROWS_ONE, get), real, imag)
    real, imag = cross(real, imag, get(3, 6), 6, 0, True)
    real, imag = pair_op(times_on_lanes, lane_operator(product(A_ONE_LATE, LANES_ONE, get)), real, imag)
    real, imag = pair_op(times_from_left, product(B_ONE_LATE, ROWS_ONE, get), real, imag)
    real, imag = cross(real, imag, get(6, 6), 6, 0, True)
    pairs = ((3, 6), (2, 5), (1, 4))
    real, imag = exchanged(real, pairs), exchanged(imag, pairs)
    for v in range(VREGS):
        out_ref[pl.ds(16 * v, SUBLANES, stride=2), :] = real[v]
        out_ref[pl.ds(16 * v + 1, SUBLANES, stride=2), :] = imag[v]


def stage_two(x_ref, gates_ref, out_ref, scratch):
    get = getter(gates_ref, scratch)
    real = [x_ref[pl.ds(16 * v, SUBLANES, stride=2), :] for v in range(VREGS)]
    imag = [x_ref[pl.ds(16 * v + 1, SUBLANES, stride=2), :] for v in range(VREGS)]
    pairs = ((1, 6), (2, 5), (3, 4))
    real, imag = exchanged(real, pairs), exchanged(imag, pairs)
    order = [((v << 1) & 15) | (v >> 3) for v in range(VREGS)]
    real, imag = [real[o] for o in order], [imag[o] for o in order]
    real, imag = cross(real, imag, get(1, 17), 6, 6, False)
    real, imag = pair_op(times_on_lanes, lane_operator(product(A_TWO, LANES_TWO, get)), real, imag)
    real, imag = pair_op(times_from_left, product(B_TWO, ROWS_TWO, get), real, imag)
    real, imag = cross(real, imag, get(4, 17), 6, 6, False)
    real, imag = pair_op(times_from_left, product(B_TWO_LATE, ROWS_TWO, get), real, imag)
    late = lane_operator(product(A_TWO_LATE, LANES_TWO, get))
    real, imag = pair_op(times_on_lanes_transposed, late, real, imag)
    real, imag = cross(real, imag, get(7, 17), 6, 6, True)
    for v in range(VREGS):
        three, q20, q19, q18 = v & 1, (v >> 1) & 1, (v >> 2) & 1, v >> 3
        at = 32 * (8 * three + 4 * q20 + 2 * q19 + q18) + 16
        out_ref[at : at + 8, :] = real[v]
        out_ref[at + 8 : at + 16, :] = imag[v]
    for three in range(2):
        for part in range(2):
            for low in range(SUBLANES):
                to = 32 * (8 * three + low) + 8 * part
                rows = out_ref[pl.ds(256 * three + 16 + 8 * part + low, SUBLANES, stride=32), :]
                out_ref[to : to + 8, :] = rows


def stage_three(x_ref, gates_ref, state_ref, marginal_ref, scratch):
    get = getter(gates_ref, scratch)
    operator = lane_operator(product(D_THREE, LANES_THREE, get, LANES_LAST))
    pairs = ((3, 6), (2, 2), (1, 1), (0, 0))
    for layout in range(2):
        real = [x_ref[32 * v + 16 * layout : 32 * v + 16 * layout + 8, :] for v in range(VREGS)]
        imag = [x_ref[32 * v + 16 * layout + 8 : 32 * v + 16 * layout + 16, :] for v in range(VREGS)]
        real, imag = exchanged(real, pairs), exchanged(imag, pairs)
        real, imag = pair_op(times_on_lanes, operator, real, imag)
        for v in range(VREGS):
            if layout == 0:
                state_ref[pl.ds(2 * v, SUBLANES, stride=32), :] = real[v]
                state_ref[pl.ds(2 * v + 1, SUBLANES, stride=32), :] = imag[v]
            else:
                prob = real[v] * real[v] + imag[v] * imag[v]
                marginal_ref[v : v + 1, :] = jnp.sum(prob, axis=0, keepdims=True)


INTERPRET = False


def run(kernel, shapes, x, gates, name):
    return pl.pallas_call(
        kernel,
        out_shape=[jax.ShapeDtypeStruct(shape, jnp.float32) for shape in shapes],
        scratch_shapes=[pltpu.VMEM(TILE, jnp.float32)],
        name=name,
        interpret=INTERPRET,
    )(x, gates)


def first(x, gates):
    return run(stage_one, [(256, LANES)], x, gates, "stage_one")[0]


def second(x, gates):
    return run(stage_two, [(512, LANES)], x, gates, "stage_two")[0]


def third(x, gates):
    return run(stage_three, [(256, LANES), (16, LANES)], x, gates, "stage_three")


def local(state, gates):
    amplitudes = state.shape[-1]
    rows = amplitudes // LANES
    matrices = gates.reshape(-1, *gates.shape[-2:])
    x = state.reshape(2, rows, LANES).transpose(1, 0, 2).reshape(2 * rows, LANES)
    x = first(x, matrices)
    x = lax.all_to_all(x, ("high", "core", "narrow"), 0, 0, tiled=True)
    x = second(x, matrices)
    x = lax.all_to_all(x, ("core", "narrow"), 0, 0, tiled=True)
    final, marginal = third(x, matrices)
    final = final.reshape(rows, 2, LANES).transpose(1, 0, 2)
    return final.reshape(1, 1, 2, amplitudes), marginal.reshape(1, -1)


def solution(mesh):
    slices, wide, narrow = mesh.devices.shape
    devices = mesh.devices.reshape(slices, wide // 2, 2, narrow)
    split = Mesh(devices, ("slices", "high", "core", "narrow"))
    over_wide = ("slices", "high", "core")
    spec = P(over_wide, "narrow", None, None)
    return jax.shard_map(
        local, mesh=split, in_specs=(spec, P()), out_specs=(spec, P(over_wide, "narrow")), check_vma=False
    )
```

```python
import jax
import jax.numpy as jnp
from jax import lax
from jax.experimental import pallas as pl
from jax.experimental.pallas import tpu as pltpu
from jax.sharding import Mesh, PartitionSpec as P

RING = 21
STEP = 7
VREGS = 16
SUBLANES = 8
LANES = 128
TILE = (SUBLANES, LANES)


def lane_iota():
    return lax.broadcasted_iota(jnp.int32, TILE, 1)


def sublane_iota():
    return lax.broadcasted_iota(jnp.int32, TILE, 0)


def bit_of(array, place):
    return (array >> place) & 1


def splits(array):
    high = array.astype(jnp.bfloat16)
    low = (array - high.astype(jnp.float32)).astype(jnp.bfloat16)
    return high, low


def dot(a, b, dims):
    return lax.dot_general(a, b, (dims, ((), ())), preferred_element_type=jnp.float32)


def dot_three(a, b, dims):
    return dot(a[0], b[0], dims) + dot(a[0], b[1], dims) + dot(a[1], b[0], dims)


def stack(parts):
    return jnp.concatenate(parts, axis=0)


def beside(left, right):
    return tuple(jnp.concatenate([l, r], axis=1) for l, r in zip(left, right))


def over(top, bottom):
    return tuple(jnp.concatenate([t, b], axis=0) for t, b in zip(top, bottom))


def negative(parts):
    return tuple(-part for part in parts)


def unstack(array):
    return [array[SUBLANES * v : SUBLANES * (v + 1)] for v in range(array.shape[0] // SUBLANES)]


def times_from_left(matrix, real, imag):
    left = beside(splits(matrix[0]), splits(matrix[1]))
    re, im = splits(real), splits(imag)
    right = over(beside(re, im), beside(negative(im), re))
    out = dot_three(left, right, ((1,), (0,)))
    return out[:, :LANES], out[:, LANES:]


def lane_operator(matrix):
    re, im = splits(matrix[0]), splits(matrix[1])
    return over(beside(re, negative(im)), beside(im, re))


def times_on_lanes(operator, real, imag):
    out = dot_three(beside(splits(real), splits(imag)), operator, ((1,), (1,)))
    return out[:, :LANES], out[:, LANES:]


def times_on_lanes_transposed(operator, real, imag):
    out = dot_three(operator, beside(splits(real), splits(imag)), ((1,), (1,)))
    return out[:LANES], out[LANES:]


def gate_tiles(gates_ref):
    rows = gates_ref.shape[0]
    tail = jnp.concatenate([gates_ref[LANES:, :], jnp.zeros((2 * LANES - rows, SUBLANES), jnp.float32)], axis=0)
    return gates_ref[:LANES, :].T, tail.T


def spread(tile, row):
    return jnp.broadcast_to(tile[row : row + 1, :], TILE)


def column_tile(gate, column):
    tile, base = gate
    return jnp.take_along_axis(tile, base + 4 * sublane_iota() + column, axis=1)


def brick(gates, ins, outs):
    lane, sub = lane_iota(), sublane_iota()
    touched, factors = set(), []
    for table, low in gates:
        high = (low + 1) % RING
        touched |= {low, high}
        column = bit_of(lane, ins[low]) + 2 * bit_of(lane, ins[high])
        wide = column_tile(table, column)
        factors.append((low, high, [(spread(wide, r), spread(wide, 4 + r)) for r in range(4)]))
    cache = {}

    def static(place, v):
        return None if place < 3 else (v >> (place - 3)) & 1

    def pick(place, v, zero, one):
        if place >= 3:
            return one if static(place, v) else zero
        mask = bit_of(sub, place) == 1
        return tuple(jnp.where(mask, o, z) for z, o in zip(zero, one))

    def entry(index, v):
        low, high, rows = factors[index]
        key = (index, static(outs[low], v), static(outs[high], v))
        if key not in cache:
            zero = pick(outs[low], v, rows[0], rows[1])
            one = pick(outs[low], v, rows[2], rows[3])
            cache[key] = pick(outs[high], v, zero, one)
        return cache[key], key

    real, imag = [], []
    for v in range(VREGS):
        value, key = entry(0, v)
        key = (key,)
        for index in range(1, len(factors)):
            other, own = entry(index, v)
            key = key + (own,)
            if key not in cache:
                (a, b), (c, d) = value, other
                cache[key] = (a * c - b * d, a * d + b * c)
            value = cache[key]
        mask = None
        for qubit in ins:
            if qubit in touched:
                continue
            place = outs[qubit]
            bit = bit_of(lane, ins[qubit])
            same = (bit == bit_of(sub, place)) if place < 3 else (bit == static(place, v))
            mask = same if mask is None else mask & same
        if mask is not None:
            value = tuple(jnp.where(mask, part, 0.0) for part in value)
        real.append(value[0])
        imag.append(value[1])
    return stack(real), stack(imag)


def product(layers, places, get, outs=None):
    matrix = None
    for number, layer in enumerate(layers):
        last = number == len(layers) - 1
        step = brick([(get(*g), g[1]) for g in layer], places, outs if outs and last else places)
        matrix = step if matrix is None else times_from_left(step, *matrix)
    return matrix


def flip_lanes(tile, place):
    width = 1 << place
    if 2 * width == LANES:
        return pltpu.roll(tile, width, 1)
    lane = lane_iota()
    return jnp.where(bit_of(lane, place) == 1, pltpu.roll(tile, width, 1), pltpu.roll(tile, LANES - width, 1))


def flip_rows(tiles, place):
    if place >= 3:
        return [tiles[v ^ (1 << (place - 3))] for v in range(VREGS)]
    width = 1 << place
    up = bit_of(sublane_iota(), place) == 1
    return [jnp.where(up, pltpu.roll(t, width, 0), pltpu.roll(t, SUBLANES - width, 0)) for t in tiles]


def cross(real, imag, table, lane_place, row_place, lane_is_low):
    lane, sub = lane_iota(), sublane_iota()
    lane_bit = bit_of(lane, lane_place)
    lane_weight, row_weight = (1, 2) if lane_is_low else (2, 1)

    def coefficient(row_value, row_flip, lane_flip):
        column = lane_weight * (lane_bit ^ lane_flip) + row_weight * (row_value ^ row_flip)
        wide = column_tile(table, column)
        base = row_weight * row_value
        return tuple(
            jnp.where(lane_bit == 1, spread(wide, shift + base + lane_weight), spread(wide, shift + base))
            for shift in (0, 4)
        )

    def coefficients(row_value):
        return {(r, l): coefficient(row_value, r, l) for r in (0, 1) for l in (0, 1)}

    both = [coefficients(0), coefficients(1)]
    if row_place < 3:
        mask = bit_of(sub, row_place) == 1
        mixed = {k: tuple(jnp.where(mask, o, z) for z, o in zip(both[0][k], both[1][k])) for k in both[0]}
    inputs = {}
    for l in (0, 1):
        re = [flip_lanes(t, lane_place) for t in real] if l else real
        im = [flip_lanes(t, lane_place) for t in imag] if l else imag
        for r in (0, 1):
            inputs[r, l] = (flip_rows(re, row_place), flip_rows(im, row_place)) if r else (re, im)
    out_real, out_imag = [], []
    for v in range(VREGS):
        factors = mixed if row_place < 3 else both[(v >> (row_place - 3)) & 1]
        re = im = None
        for key, (c, d) in factors.items():
            a, b = inputs[key][0][v], inputs[key][1][v]
            re = a * c - b * d if re is None else re + a * c - b * d
            im = a * d + b * c if im is None else im + a * d + b * c
        out_real.append(re)
        out_imag.append(im)
    return out_real, out_imag


def exchanged(tiles, pairs):
    lane = lane_iota()
    for register, place in pairs:
        width = 1 << place
        upper = bit_of(lane, place) == 1
        result = list(tiles)
        for v in range(VREGS):
            if (v >> register) & 1:
                continue
            other = v | (1 << register)
            a, b = tiles[v], tiles[other]
            result[v] = jnp.where(upper, pltpu.roll(b, width, 1), a)
            result[other] = jnp.where(upper, b, pltpu.roll(a, LANES - width, 1))
        tiles = result
    return tiles


def places_of(qubits):
    return {q: place for place, q in enumerate(qubits)}


LANES_ONE, ROWS_ONE = places_of(range(0, 7)), places_of(range(7, 14))
LANES_TWO, ROWS_TWO = places_of([0, 1, 2, 3, 20, 19, 18]), places_of([14, 15, 16, 13, 12, 11, 17])
LANES_THREE, LANES_LAST = places_of([7, 8, 9, 13, 12, 11, 10]), places_of(range(7, 14))


def layers_of(*layers):
    return [[(layer, low) for layer, low in group] for group in layers]


A_ONE = layers_of(
    [(0, 0), (0, 2), (0, 4)], [(2, 1), (2, 3), (2, 5)], [(3, 2), (3, 4)], [(5, 3)]
)
B_ONE = layers_of(
    [(0, 8), (0, 10), (0, 12)], [(1, 7), (1, 9), (1, 11)], [(3, 8), (3, 10)], [(4, 9)]
)
A_ONE_LATE = layers_of([(5, 5)], [(6, 4)])
B_ONE_LATE = layers_of([(4, 7)], [(6, 8)])
A_TWO = layers_of([(1, 19)], [(2, 18), (2, 20)], [(4, 19), (3, 0)])
B_TWO = layers_of(
    [(1, 13), (1, 15)], [(2, 14), (2, 16), (3, 12)], [(4, 11), (4, 13), (4, 15)]
)
A_TWO_LATE = layers_of([(5, 18), (5, 20), (5, 1)], [(7, 19), (6, 0), (6, 2)])
B_TWO_LATE = layers_of([(5, 14), (5, 16), (6, 12)], [(7, 13), (7, 15)])
D_THREE = layers_of([(6, 10)], [(7, 9), (7, 11), (7, 7)])


def getter(gates_ref):
    tiles = gate_tiles(gates_ref)

    def get(layer, low):
        pair = ((low - layer * STEP) % RING) // 2
        return spread(tiles[pair // 4], layer), 32 * (pair % 4)

    return get


def pair_op(op, matrix, real, imag):
    re, im = op(matrix, stack(real), stack(imag))
    return unstack(re), unstack(im)


def stage_one(x_ref, gates_ref, out_ref):
    get = getter(gates_ref)
    real = [x_ref[pl.ds(16 * v, SUBLANES, stride=2), :] for v in range(VREGS)]
    imag = [x_ref[pl.ds(16 * v + 1, SUBLANES, stride=2), :] for v in range(VREGS)]
    real, imag = cross(real, imag, get(0, 6), 6, 0, True)
    real, imag = pair_op(times_on_lanes, lane_operator(product(A_ONE, LANES_ONE, get)), real, imag)
    real, imag = pair_op(times_from_left, product(B_ONE, ROWS_ONE, get), real, imag)
    real, imag = cross(real, imag, get(3, 6), 6, 0, True)
    real, imag = pair_op(times_on_lanes, lane_operator(product(A_ONE_LATE, LANES_ONE, get)), real, imag)
    real, imag = pair_op(times_from_left, product(B_ONE_LATE, ROWS_ONE, get), real, imag)
    real, imag = cross(real, imag, get(6, 6), 6, 0, True)
    pairs = ((3, 6), (2, 5), (1, 4))
    real, imag = exchanged(real, pairs), exchanged(imag, pairs)
    for v in range(VREGS):
        out_ref[pl.ds(16 * v, SUBLANES, stride=2), :] = real[v]
        out_ref[pl.ds(16 * v + 1, SUBLANES, stride=2), :] = imag[v]


def stage_two(x_ref, gates_ref, out_ref):
    get = getter(gates_ref)
    real = [x_ref[pl.ds(16 * v, SUBLANES, stride=2), :] for v in range(VREGS)]
    imag = [x_ref[pl.ds(16 * v + 1, SUBLANES, stride=2), :] for v in range(VREGS)]
    pairs = ((1, 6), (2, 5), (3, 4))
    real, imag = exchanged(real, pairs), exchanged(imag, pairs)
    order = [((v << 1) & 15) | (v >> 3) for v in range(VREGS)]
    real, imag = [real[o] for o in order], [imag[o] for o in order]
    real, imag = cross(real, imag, get(1, 17), 6, 6, False)
    real, imag = pair_op(times_on_lanes, lane_operator(product(A_TWO, LANES_TWO, get)), real, imag)
    real, imag = pair_op(times_from_left, product(B_TWO, ROWS_TWO, get), real, imag)
    real, imag = cross(real, imag, get(4, 17), 6, 6, False)
    real, imag = pair_op(times_from_left, product(B_TWO_LATE, ROWS_TWO, get), real, imag)
    late = lane_operator(product(A_TWO_LATE, LANES_TWO, get))
    real, imag = pair_op(times_on_lanes_transposed, late, real, imag)
    real, imag = cross(real, imag, get(7, 17), 6, 6, True)
    for v in range(VREGS):
        three, q20, q19, q18 = v & 1, (v >> 1) & 1, (v >> 2) & 1, v >> 3
        at = 32 * (8 * three + 4 * q20 + 2 * q19 + q18) + 16
        out_ref[at : at + 8, :] = real[v]
        out_ref[at + 8 : at + 16, :] = imag[v]
    for three in range(2):
        for part in range(2):
            for low in range(SUBLANES):
                to = 32 * (8 * three + low) + 8 * part
                rows = out_ref[pl.ds(256 * three + 16 + 8 * part + low, SUBLANES, stride=32), :]
                out_ref[to : to + 8, :] = rows


def stage_three(x_ref, gates_ref, state_ref, marginal_ref):
    get = getter(gates_ref)
    operator = lane_operator(product(D_THREE, LANES_THREE, get, LANES_LAST))
    pairs = ((3, 6), (2, 2), (1, 1), (0, 0))
    for layout in range(2):
        real = [x_ref[32 * v + 16 * layout : 32 * v + 16 * layout + 8, :] for v in range(VREGS)]
        imag = [x_ref[32 * v + 16 * layout + 8 : 32 * v + 16 * layout + 16, :] for v in range(VREGS)]
        real, imag = exchanged(real, pairs), exchanged(imag, pairs)
        real, imag = pair_op(times_on_lanes, operator, real, imag)
        for v in range(VREGS):
            if layout == 0:
                state_ref[pl.ds(2 * v, SUBLANES, stride=32), :] = real[v]
                state_ref[pl.ds(2 * v + 1, SUBLANES, stride=32), :] = imag[v]
            else:
                prob = real[v] * real[v] + imag[v] * imag[v]
                marginal_ref[v : v + 1, :] = jnp.sum(prob, axis=0, keepdims=True)


INTERPRET = False
VMEM_LIMIT = 8 << 20


def run(kernel, shapes, x, gates, name):
    return pl.pallas_call(
        kernel,
        out_shape=[jax.ShapeDtypeStruct(shape, jnp.float32) for shape in shapes],
        compiler_params=pltpu.CompilerParams(vmem_limit_bytes=VMEM_LIMIT),
        name=name,
        interpret=INTERPRET,
    )(x, gates)


def first(x, gates):
    return run(stage_one, [(256, LANES)], x, gates, "stage_one")[0]


def second(x, gates):
    return run(stage_two, [(512, LANES)], x, gates, "stage_two")[0]


def third(x, gates):
    return run(stage_three, [(256, LANES), (16, LANES)], x, gates, "stage_three")


def local(state, gates):
    amplitudes = state.shape[-1]
    rows = amplitudes // LANES
    matrices = gates.transpose(1, 2, 3, 4, 0).reshape(-1, gates.shape[0])
    x = state.reshape(2, rows, LANES).transpose(1, 0, 2).reshape(2 * rows, LANES)
    x = first(x, matrices)
    x = lax.all_to_all(x, ("high", "core", "narrow"), 0, 0, tiled=True)
    x = second(x, matrices)
    x = lax.all_to_all(x, ("core", "narrow"), 0, 0, tiled=True)
    final, marginal = third(x, matrices)
    final = final.reshape(rows, 2, LANES).transpose(1, 0, 2)
    return final.reshape(1, 1, 2, amplitudes), marginal.reshape(1, -1)


def solution(mesh):
    slices, wide, narrow = mesh.devices.shape
    devices = mesh.devices.reshape(slices, wide // 2, 2, narrow)
    split = Mesh(devices, ("slices", "high", "core", "narrow"))
    over_wide = ("slices", "high", "core")
    spec = P(over_wide, "narrow", None, None)
    return jax.shard_map(
        local, mesh=split, in_specs=(spec, P()), out_specs=(spec, P(over_wide, "narrow")), check_vma=False
    )
```

```python
import jax
import jax.numpy as jnp
from jax import lax
from jax.experimental import pallas as pl
from jax.experimental.pallas import tpu as pltpu
from jax.sharding import Mesh, PartitionSpec as P

RING = 21
STEP = 7
VREGS = 16
SUBLANES = 8
LANES = 128
TILE = (SUBLANES, LANES)
LEFT = ((1,), (0,))
RIGHT = ((1,), (1,))


def lane_iota():
    return lax.broadcasted_iota(jnp.int32, TILE, 1)


def sublane_iota():
    return lax.broadcasted_iota(jnp.int32, TILE, 0)


def bit_of(array, place):
    return (array >> place) & 1


def splits(array):
    high = array.astype(jnp.bfloat16)
    low = (array - high.astype(jnp.float32)).astype(jnp.bfloat16)
    return high, low


def dot(a, b, dims):
    return lax.dot_general(a, b, (dims, ((), ())), preferred_element_type=jnp.float32)


def dot_three(a, b, dims):
    return dot(a[0], b[0], dims) + dot(a[0], b[1], dims) + dot(a[1], b[0], dims)


def stack(parts):
    return jnp.concatenate(parts, axis=0)


def beside(left, right):
    return tuple(jnp.concatenate([l, r], axis=1) for l, r in zip(left, right))


def over(top, bottom):
    return tuple(jnp.concatenate([t, b], axis=0) for t, b in zip(top, bottom))


def negative(parts):
    return tuple(-part for part in parts)


def unstack(array):
    return [array[SUBLANES * v : SUBLANES * (v + 1)] for v in range(array.shape[0] // SUBLANES)]


def row_operator(matrix):
    return beside(splits(matrix[0]), splits(matrix[1]))


def lane_operator(matrix):
    re, im = splits(matrix[0]), splits(matrix[1])
    return over(beside(re, negative(im)), beside(im, re))


def times_on_rows(operator, real, imag):
    re, im = splits(real), splits(imag)
    out = dot_three(operator, over(beside(re, im), beside(negative(im), re)), LEFT)
    return out[:, :LANES], out[:, LANES:]


def times_on_lanes(operator, real, imag):
    out = dot_three(beside(splits(real), splits(imag)), operator, RIGHT)
    return out[:, :LANES], out[:, LANES:]


def times_on_lanes_transposed(operator, real, imag):
    out = dot_three(operator, beside(splits(real), splits(imag)), RIGHT)
    return out[:LANES], out[LANES:]


def gate_tiles(gates_ref):
    rows = gates_ref.shape[0]
    tail = jnp.concatenate([gates_ref[LANES:, :], jnp.zeros((2 * LANES - rows, SUBLANES), jnp.float32)], axis=0)
    return gates_ref[:LANES, :].T, tail.T


def column_tile(gate, column):
    tile, base = gate
    return jnp.take_along_axis(tile, base + 4 * sublane_iota() + column, axis=1)


def spread(tile, row):
    return jnp.broadcast_to(tile[row : row + 1, :], TILE)


def getter(gates_ref):
    tiles = gate_tiles(gates_ref)

    def get(layer, low):
        pair = ((low - layer * STEP) % RING) // 2
        return spread(tiles[pair // 4], layer), 32 * (pair % 4)

    return get


def brick(gates, ins, outs):
    lane, sub = lane_iota(), sublane_iota()
    touched, factors = set(), []
    for gate, low in gates:
        high = (low + 1) % RING
        touched |= {low, high}
        wide = column_tile(gate, bit_of(lane, ins[low]) + 2 * bit_of(lane, ins[high]))
        factors.append((low, high, [(spread(wide, r), spread(wide, 4 + r)) for r in range(4)]))
    cache = {}

    def static(place, v):
        return None if place < 3 else (v >> (place - 3)) & 1

    def pick(place, v, zero, one):
        if place >= 3:
            return one if static(place, v) else zero
        mask = bit_of(sub, place) == 1
        return tuple(jnp.where(mask, o, z) for z, o in zip(zero, one))

    def entry(index, v):
        low, high, rows = factors[index]
        key = (index, static(outs[low], v), static(outs[high], v))
        if key not in cache:
            zero = pick(outs[low], v, rows[0], rows[1])
            one = pick(outs[low], v, rows[2], rows[3])
            cache[key] = pick(outs[high], v, zero, one)
        return cache[key], key

    real, imag = [], []
    for v in range(VREGS):
        value, key = entry(0, v)
        key = (key,)
        for index in range(1, len(factors)):
            other, own = entry(index, v)
            key = key + (own,)
            if key not in cache:
                (a, b), (c, d) = value, other
                cache[key] = (a * c - b * d, a * d + b * c)
            value = cache[key]
        mask = None
        for qubit in ins:
            if qubit in touched:
                continue
            place = outs[qubit]
            bit = bit_of(lane, ins[qubit])
            same = (bit == bit_of(sub, place)) if place < 3 else (bit == static(place, v))
            mask = same if mask is None else mask & same
        if mask is not None:
            value = tuple(jnp.where(mask, part, 0.0) for part in value)
        real.append(value[0])
        imag.append(value[1])
    return stack(real), stack(imag)


def products(get, *groups):
    chains = []
    for layers, ins, outs in groups:
        last = len(layers) - 1
        chains.append(
            [brick([(get(*g), g[1]) for g in layer], ins, outs if n == last else ins) for n, layer in enumerate(layers)]
        )
    while any(len(chain) > 1 for chain in chains):
        for number, chain in enumerate(chains):
            joined = [
                times_on_rows(row_operator(chain[i + 1]), *chain[i]) if i + 1 < len(chain) else chain[i]
                for i in range(0, len(chain), 2)
            ]
            chains[number] = joined
    return [chain[0] for chain in chains]


def flip_lanes(tile, place):
    width = 1 << place
    if 2 * width == LANES:
        return pltpu.roll(tile, width, 1)
    lane = lane_iota()
    return jnp.where(bit_of(lane, place) == 1, pltpu.roll(tile, width, 1), pltpu.roll(tile, LANES - width, 1))


def flip_rows(tiles, place):
    if place >= 3:
        return [tiles[v ^ (1 << (place - 3))] for v in range(VREGS)]
    width = 1 << place
    up = bit_of(sublane_iota(), place) == 1
    return [jnp.where(up, pltpu.roll(t, width, 0), pltpu.roll(t, SUBLANES - width, 0)) for t in tiles]


FLIPS = ((0, 0), (0, 1), (1, 0), (1, 1))


def cross_coefficients(gate, lane_place, row_place, lane_is_low):
    lane_bit = bit_of(lane_iota(), lane_place)
    lane_weight, row_weight = (1, 2) if lane_is_low else (2, 1)

    def coefficient(row_value, row_flip, lane_flip):
        column = lane_weight * (lane_bit ^ lane_flip) + row_weight * (row_value ^ row_flip)
        wide = column_tile(gate, column)
        base = row_weight * row_value
        return tuple(
            jnp.where(lane_bit == 1, spread(wide, shift + base + lane_weight), spread(wide, shift + base))
            for shift in (0, 4)
        )

    both = [[coefficient(value, *flips) for flips in FLIPS] for value in (0, 1)]
    if row_place < 3:
        mask = bit_of(sublane_iota(), row_place) == 1
        mixed = [tuple(jnp.where(mask, o, z) for z, o in zip(*pair)) for pair in zip(*both)]
        return [mixed, mixed]
    return both


def cross(real, imag, factors, lane_place, row_place):
    inputs = []
    lanes = (real, imag), tuple([flip_lanes(t, lane_place) for t in part] for part in (real, imag))
    for row_flip, lane_flip in FLIPS:
        parts = lanes[lane_flip]
        inputs.append(tuple(flip_rows(part, row_place) for part in parts) if row_flip else parts)
    out_real, out_imag = [], []
    for v in range(VREGS):
        re = im = None
        for (c, d), (xs, ys) in zip(factors[(v >> (row_place - 3)) & 1 if row_place >= 3 else 0], inputs):
            a, b = xs[v], ys[v]
            re = a * c - b * d if re is None else re + a * c - b * d
            im = a * d + b * c if im is None else im + a * d + b * c
        out_real.append(re)
        out_imag.append(im)
    return out_real, out_imag


def exchanged(tiles, pairs):
    lane = lane_iota()
    uppers = [bit_of(lane, place) == 1 for _, place in pairs]
    count = 1 << len(pairs)
    result = []
    for v in range(VREGS):
        base, shift = v, 0
        for register, place in pairs:
            if (v >> register) & 1:
                base ^= 1 << register
                shift -= 1 << place
        parts = []
        for group in range(count):
            source, move = base, shift
            for number, (register, place) in enumerate(pairs):
                if (group >> number) & 1:
                    source |= 1 << register
                    move += 1 << place
            move %= LANES
            parts.append(pltpu.roll(tiles[source], move, 1) if move else tiles[source])
        for upper in uppers:
            parts = [jnp.where(upper, parts[i + 1], parts[i]) for i in range(0, len(parts), 2)]
        result.append(parts[0])
    return result


def places_of(qubits):
    return {q: place for place, q in enumerate(qubits)}


LANES_ONE, ROWS_ONE = places_of(range(0, 7)), places_of(range(7, 14))
LANES_TWO, ROWS_TWO = places_of([0, 1, 2, 3, 20, 19, 18]), places_of([14, 15, 16, 13, 12, 11, 17])
LANES_THREE, LANES_LAST = places_of([7, 8, 9, 13, 12, 11, 10]), places_of(range(7, 14))

A_ONE = [[(0, 0), (0, 2), (0, 4)], [(2, 1), (2, 3), (2, 5)], [(3, 2), (3, 4)], [(5, 3)]]
B_ONE = [[(0, 8), (0, 10), (0, 12)], [(1, 7), (1, 9), (1, 11)], [(3, 8), (3, 10)], [(4, 9)]]
A_ONE_LATE = [[(5, 5)], [(6, 4)]]
B_ONE_LATE = [[(4, 7)], [(6, 8)]]
A_TWO = [[(1, 19)], [(2, 18), (2, 20)], [(4, 19), (3, 0)]]
B_TWO = [[(1, 13), (1, 15)], [(2, 14), (2, 16), (3, 12)], [(4, 11), (4, 13), (4, 15)]]
A_TWO_LATE = [[(5, 18), (5, 20), (5, 1)], [(7, 19), (6, 0), (6, 2)]]
B_TWO_LATE = [[(5, 14), (5, 16), (6, 12)], [(7, 13), (7, 15)]]
D_THREE = [[(6, 10)], [(7, 9), (7, 11), (7, 7)]]


def pair_op(op, operator, real, imag):
    re, im = op(operator, stack(real), stack(imag))
    return unstack(re), unstack(im)


def rows_of(ref):
    return (
        [ref[pl.ds(16 * v, SUBLANES, stride=2), :] for v in range(VREGS)],
        [ref[pl.ds(16 * v + 1, SUBLANES, stride=2), :] for v in range(VREGS)],
    )


def stage_one(state_ref, gates_hbm, out_ref, x_ref, gates_ref, semaphores):
    gates_copy = pltpu.make_async_copy(gates_hbm, gates_ref, semaphores.at[0])
    state_copy = pltpu.make_async_copy(state_ref, x_ref, semaphores.at[1])
    gates_copy.start()
    state_copy.start()
    gates_copy.wait()
    state_copy.wait()
    get = getter(gates_ref)
    lanes, rows = (LANES_ONE, LANES_ONE), (ROWS_ONE, ROWS_ONE)
    a, b, a_late, b_late = products(
        get, (A_ONE, *lanes), (B_ONE, *rows), (A_ONE_LATE, *lanes), (B_ONE_LATE, *rows)
    )
    real, imag = rows_of(x_ref)
    real, imag = cross(real, imag, cross_coefficients(get(0, 6), 6, 0, True), 6, 0)
    real, imag = pair_op(times_on_lanes, lane_operator(a), real, imag)
    real, imag = pair_op(times_on_rows, row_operator(b), real, imag)
    real, imag = cross(real, imag, cross_coefficients(get(3, 6), 6, 0, True), 6, 0)
    real, imag = pair_op(times_on_lanes, lane_operator(a_late), real, imag)
    real, imag = pair_op(times_on_rows, row_operator(b_late), real, imag)
    real, imag = cross(real, imag, cross_coefficients(get(6, 6), 6, 0, True), 6, 0)
    pairs = ((3, 6), (2, 5), (1, 4))
    real, imag = exchanged(real, pairs), exchanged(imag, pairs)
    for v in range(VREGS):
        out_ref[pl.ds(16 * v, SUBLANES, stride=2), :] = real[v]
        out_ref[pl.ds(16 * v + 1, SUBLANES, stride=2), :] = imag[v]


CROSSES_TWO = (((1, 17), False), ((4, 17), False), ((7, 17), True))


def operators(gates_ref, after_ref, a_ref, b_ref, a_late_ref, b_late_ref, d_ref, factors_ref):
    get = getter(gates_ref)
    lanes, rows = (LANES_TWO, LANES_TWO), (ROWS_TWO, ROWS_TWO)
    a, b, a_late, b_late, d = products(
        get,
        (A_TWO, *lanes),
        (B_TWO, *rows),
        (A_TWO_LATE, *lanes),
        (B_TWO_LATE, *rows),
        (D_THREE, LANES_THREE, LANES_LAST),
    )
    for ref, value in (
        (a_ref, lane_operator(a)),
        (b_ref, row_operator(b)),
        (a_late_ref, lane_operator(a_late)),
        (b_late_ref, row_operator(b_late)),
        (d_ref, lane_operator(d)),
    ):
        for part in range(2):
            ref[part] = value[part]
    at = 0
    for gate, lane_is_low in CROSSES_TWO:
        for value in cross_coefficients(get(*gate), 6, 6, lane_is_low):
            for pair in value:
                for tile in pair:
                    factors_ref[at : at + SUBLANES, :] = tile
                    at += SUBLANES


def factors_of(ref, number):
    tiles = iter(ref[at : at + SUBLANES, :] for at in range(LANES * number, LANES * (number + 1), SUBLANES))
    return [[(next(tiles), next(tiles)) for _ in FLIPS] for _ in range(2)]


def stage_two(x_ref, a_ref, b_ref, a_late_ref, b_late_ref, factors_ref, out_ref):
    real, imag = rows_of(x_ref)
    pairs = ((1, 6), (2, 5), (3, 4))
    real, imag = exchanged(real, pairs), exchanged(imag, pairs)
    order = [((v << 1) & 15) | (v >> 3) for v in range(VREGS)]
    real, imag = [real[o] for o in order], [imag[o] for o in order]
    real, imag = cross(real, imag, factors_of(factors_ref, 0), 6, 6)
    real, imag = pair_op(times_on_lanes, (a_ref[0], a_ref[1]), real, imag)
    real, imag = pair_op(times_on_rows, (b_ref[0], b_ref[1]), real, imag)
    real, imag = cross(real, imag, factors_of(factors_ref, 1), 6, 6)
    real, imag = pair_op(times_on_rows, (b_late_ref[0], b_late_ref[1]), real, imag)
    real, imag = pair_op(times_on_lanes_transposed, (a_late_ref[0], a_late_ref[1]), real, imag)
    real, imag = cross(real, imag, factors_of(factors_ref, 2), 6, 6)
    for v in range(VREGS):
        three, q20, q19, q18 = v & 1, (v >> 1) & 1, (v >> 2) & 1, v >> 3
        at = 32 * (8 * three + 4 * q20 + 2 * q19 + q18) + 16
        out_ref[at : at + 8, :] = real[v]
        out_ref[at + 8 : at + 16, :] = imag[v]
    for three in range(2):
        for part in range(2):
            for low in range(SUBLANES):
                to = 32 * (8 * three + low) + 8 * part
                rows = out_ref[pl.ds(256 * three + 16 + 8 * part + low, SUBLANES, stride=32), :]
                out_ref[to : to + 8, :] = rows


def stage_three(x_ref, d_ref, state_hbm, marginal_hbm, state_ref, marginal_ref, semaphores):
    copies = (
        pltpu.make_async_copy(state_ref, state_hbm, semaphores.at[0]),
        pltpu.make_async_copy(marginal_ref, marginal_hbm, semaphores.at[1]),
    )
    for layout in range(2):
        at = [32 * v + 16 * layout for v in range(VREGS)]
        real = [x_ref[a : a + 8, :] for a in at]
        imag = [x_ref[a + 8 : a + 16, :] for a in at]
        for pairs in (((3, 6), (2, 2)), ((1, 1), (0, 0))):
            real, imag = exchanged(real, pairs), exchanged(imag, pairs)
        real, imag = pair_op(times_on_lanes, (d_ref[0], d_ref[1]), real, imag)
        for v in range(VREGS):
            if layout == 0:
                state_ref[pl.ds(2 * v, SUBLANES, stride=32), :] = real[v]
                state_ref[pl.ds(2 * v + 1, SUBLANES, stride=32), :] = imag[v]
            else:
                prob = real[v] * real[v] + imag[v] * imag[v]
                marginal_ref[v : v + 1, :] = jnp.sum(prob, axis=0, keepdims=True)
        copies[layout].start()
    for copy in copies:
        copy.wait()


INTERPRET = False
VMEM_LIMIT = 8 << 20
HBM = pl.BlockSpec(memory_space=pltpu.HBM)
VMEM = pl.BlockSpec(memory_space=pltpu.VMEM)


def run(kernel, outs, args, ins, out_specs, scratch=(), flops=1000000):
    return pl.pallas_call(
        kernel,
        out_shape=outs,
        in_specs=ins,
        out_specs=out_specs,
        scratch_shapes=scratch,
        compiler_params=pltpu.CompilerParams(vmem_limit_bytes=VMEM_LIMIT),
        cost_estimate=pl.CostEstimate(flops=flops, bytes_accessed=262144, transcendentals=0),
        name=kernel.__name__,
        interpret=INTERPRET,
    )(*args)


def array(*shape, dtype=jnp.float32):
    return jax.ShapeDtypeStruct(shape, dtype)


def first(x, gates):
    scratch = [pltpu.VMEM(x.shape, jnp.float32), pltpu.VMEM(gates.shape, jnp.float32), pltpu.SemaphoreType.DMA((2,))]
    args = (x, gates) if INTERPRET else tuple(pltpu.with_memory_space_constraint(a, pltpu.HBM) for a in (x, gates))
    return run(stage_one, array(2 * LANES, LANES), args, [HBM, HBM], VMEM, scratch)


def prepare(gates, after):
    lane = array(2, 2 * LANES, 2 * LANES, dtype=jnp.bfloat16)
    row = array(2, LANES, 2 * LANES, dtype=jnp.bfloat16)
    outs = [lane, row, lane, row, lane, array(3 * LANES, LANES)]
    ins = [VMEM, VMEM]
    return run(operators, outs, (gates, after), ins, [VMEM] * 6, flops=100000000)


def second(x, a, b, a_late, b_late, factors):
    return run(stage_two, array(4 * LANES, LANES), (x, a, b, a_late, b_late, factors), [VMEM] * 6, VMEM)


def third(x, d):
    outs = [array(2 * LANES, LANES), array(VREGS, LANES)]
    scratch = [pltpu.VMEM(out.shape, jnp.float32) for out in outs] + [pltpu.SemaphoreType.DMA((2,))]
    return run(stage_three, outs, (x, d), [VMEM, VMEM], [HBM, HBM], scratch)


def local(state, gates):
    amplitudes = state.shape[-1]
    rows = amplitudes // LANES
    matrices = gates.transpose(1, 2, 3, 4, 0).reshape(-1, gates.shape[0])
    x = state.reshape(2, rows, LANES).transpose(1, 0, 2).reshape(2 * rows, LANES)
    x = first(x, matrices)
    *two, d, factors = prepare(matrices, x)
    x = lax.all_to_all(x, ("high", "core", "narrow"), 0, 0, tiled=True)
    x = second(x, *two, factors)
    x = lax.all_to_all(x, ("core", "narrow"), 0, 0, tiled=True)
    final, marginal = third(x, d)
    final = final.reshape(rows, 2, LANES).transpose(1, 0, 2)
    return final.reshape(1, 1, 2, amplitudes), marginal.reshape(1, -1)


def solution(mesh):
    slices, wide, narrow = mesh.devices.shape
    devices = mesh.devices.reshape(slices, wide // 2, 2, narrow)
    split = Mesh(devices, ("slices", "high", "core", "narrow"))
    over_wide = ("slices", "high", "core")
    spec = P(over_wide, "narrow", None, None)
    return jax.shard_map(
        local, mesh=split, in_specs=(spec, P()), out_specs=(spec, P(over_wide, "narrow")), check_vma=False
    )
```
